32 devices in a mesh: gx: 2 (over x), gy: 4 (over y, core), gz: 4 (over z).
Axes of the slice: x: 2, y: 2, z: 4, core: 2. Of those that a mesh axis runs over, the one named last changes fastest.
Arguments:
- query: bfloat16 [4, 4, 4096], replicated, may hold values from -50 to 50
- keys: bfloat16 [4096, 4, 4096], P(('gx', 'gy', 'gz')), may hold values from -6 to 6
- values: bfloat16 [4096, 4, 4096], P(('gx', 'gy', 'gz')), may hold values from -6 to 6
- lm_keys: bfloat16 [128, 4, 4096], P(('gx', 'gy', 'gz')), may hold values from -10 to 10
- lm_values: bfloat16 [128, 4, 4096], P(('gx', 'gy', 'gz')), may hold values from -6 to 6
- selected: int32 [4, 16, 16], replicated, may hold values from 0 to 127, as said below
Outputs:
- attended: float32 [4, 4, 4096], P(None, None, ('gx', 'gy', 'gz'))
The draws below stay inside these ranges and needn't reach their ends.
Inputs may be any that keep to these rules, and one draw needn't show every extreme that they name: `selected`: each batch row and head names 16 different blocks; every shard holds either none of them or exactly 2.
All inputs are finite; a program needn't handle non-finite values.
Results may differ from the reference program's by a relative error of at most 0.0007.
Values sent between devices are 32-bit elements; how exact they have to be, the bound alone decides.
A program may use at most 64 MiB of HBM per device.

```python
import math
import jax
import jax.numpy as jnp
from jax import lax

H = 16
HD = 256
B = 4
QPOS = 4
TOK_DEV = 128
BLK = 32
TOPB = 16
CAP = 2
TOKENS = 4096
NBLK = 128
N_GX = 2
N_GY = 4
N_GZ = 4


def pick_blocks(key):
    local_blocks = TOK_DEV // BLK
    device_count = NBLK // local_blocks
    group_count = TOPB // CAP
    first_key = jax.random.fold_in(key, 101)
    second_key = jax.random.fold_in(key, 103)
    raw_score = jax.random.randint(first_key, (B * H, device_count), 0, device_count)
    ladder = jnp.arange(device_count, dtype=jnp.int32)
    ranking = (raw_score + ladder) * device_count + ladder
    unused_values, owners = lax.top_k(ranking, group_count)
    random_rank = jax.random.randint(second_key, (B * H, group_count, local_blocks), 0, 1 << 20)
    ranked = random_rank * local_blocks + jnp.arange(local_blocks, dtype=jnp.int32)
    inner = jnp.argsort(ranked, axis=-1)[:, :, :CAP].astype(jnp.int32)
    return (owners[:, :, None].astype(jnp.int32) * local_blocks + inner).reshape(B, H, TOPB).astype(jnp.int32)


def cache_keys(key):
    draw_key = jax.random.fold_in(key, 211)
    field = jnp.clip(jax.random.normal(draw_key, (TOKENS, B, H * HD), jnp.float32), -6.0, 6.0)
    return field


def draw_keys(key, part):
    return cache_keys(key).astype(jnp.bfloat16)


def draw_selected(key, part):
    return pick_blocks(key)


def draw_query(key, part):
    draw_key = jax.random.fold_in(key, 307)
    field = jnp.clip(1.5 * jax.random.normal(draw_key, (B, QPOS, H * HD), jnp.float32), -9.0, 9.0)
    return field.astype(jnp.bfloat16)


def level_of(rng, dims, pieces, least, largest):
    def one(position, blocks):
        steps = jax.random.uniform(jax.random.fold_in(jax.random.fold_in(rng, 6), position), (blocks,), jnp.float32, least / len(pieces), largest / len(pieces))
        return jnp.repeat(jnp.exp(steps), dims[position] // blocks).reshape((-1,) + (1,) * (len(dims) - position - 1))

    factor_of = one(*pieces[0])
    for cut in pieces[1:]:
        factor_of = factor_of * one(*cut)
    return factor_of


def normal_values(rng, extent, scale, most, pieces=(), held_as=jnp.bfloat16):
    level = level_of(rng, extent, pieces, -0.22, 0.18) if pieces else 1.0
    entries = jax.random.normal(rng, extent, jnp.float32) * scale * level
    return jnp.minimum(jnp.maximum(entries, -most), most).astype(held_as)


def setup_inputs(seed: int = 0) -> dict:
    key_of = jax.random.split(jax.random.key(seed), 7)
    return {
        "query": draw_query(jax.random.fold_in(key_of[6], 71), 0),
        "keys": draw_keys(jax.random.fold_in(key_of[6], 71), 0),
        "values": normal_values(key_of[2], (TOKENS, B, H * HD), 1.0, 6.0, ((0, 32),)),
        "lm_keys": normal_values(key_of[3], (NBLK, B, H * HD), 1.7, 10.0, ((0, 32),)),
        "lm_values": normal_values(key_of[4], (NBLK, B, H * HD), 1.0, 6.0, ((0, 32),)),
        "selected": draw_selected(jax.random.fold_in(key_of[6], 71), 0),
    }


def reference(query, keys, values, lm_keys, lm_values, selected):
    shard_count = N_GX * N_GY * N_GZ
    local_blocks = TOK_DEV // BLK
    query_heads = query.reshape(B, QPOS, H, HD).astype(jnp.float32)
    score_scale = 1.0 / math.sqrt(HD)

    def shard_terms(shard):
        keys_here = lax.dynamic_slice_in_dim(keys, shard * TOK_DEV, TOK_DEV, 0).reshape(TOK_DEV, B, H, HD).astype(jnp.float32)
        values_here = lax.dynamic_slice_in_dim(values, shard * TOK_DEV, TOK_DEV, 0).reshape(TOK_DEV, B, H, HD).astype(jnp.float32)
        summary_keys = lax.dynamic_slice_in_dim(lm_keys, shard * local_blocks, local_blocks, 0).reshape(local_blocks, B, H, HD).astype(jnp.float32)
        summary_values = lax.dynamic_slice_in_dim(lm_values, shard * local_blocks, local_blocks, 0).reshape(local_blocks, B, H, HD).astype(jnp.float32)
        block_ids = shard * local_blocks + jnp.arange(local_blocks, dtype=jnp.int32)
        chosen_here = jnp.any(selected[:, :, :, None] == block_ids[None, None, None, :], axis=2)
        live_tokens = jnp.repeat(chosen_here, BLK, axis=2)
        token_score = jnp.einsum('bphd,tbhd->bpht', query_heads, keys_here) * score_scale
        token_score = jnp.where(live_tokens[:, None], token_score, -jnp.inf)
        summary_score = jnp.einsum('bphd,lbhd->bphl', query_heads, summary_keys) * score_scale
        local_peak = jnp.maximum(lax.optimization_barrier(jnp.max(token_score, -1)), lax.optimization_barrier(jnp.max(summary_score, -1)))
        token_weight = jnp.exp(token_score - local_peak[..., None])
        summary_weight = jnp.exp(summary_score - local_peak[..., None])
        local_total = lax.optimization_barrier(jnp.sum(token_weight, -1)) + lax.optimization_barrier(jnp.sum(summary_weight, -1))
        token_round = lax.optimization_barrier(token_weight.astype(jnp.bfloat16)).astype(jnp.float32)
        summary_round = lax.optimization_barrier(summary_weight.astype(jnp.bfloat16)).astype(jnp.float32)
        local_sum = jnp.einsum('bpht,tbhd->bphd', token_round, values_here) + jnp.einsum('bphl,lbhd->bphd', summary_round, summary_values)
        return (local_peak, local_total, local_sum)
    peaks, totals, sums = lax.map(shard_terms, jnp.arange(shard_count, dtype=jnp.int32))
    global_peak = lax.optimization_barrier(jnp.max(peaks, 0))
    rescale = jnp.exp(peaks - global_peak[None])
    numerator = lax.optimization_barrier(jnp.sum(rescale[..., None] * sums, 0))
    denominator = lax.optimization_barrier(jnp.sum(rescale * totals, 0))
    return (numerator / denominator[..., None]).reshape(B, QPOS, H * HD)
```

```python
import functools
import math

import jax
import jax.numpy as jnp
from jax import lax
from jax.experimental import pallas as pl
from jax.experimental.pallas import tpu as pltpu
from jax.sharding import PartitionSpec as P

AXES = ("gx", "gy", "gz")
LANES = 128
GROUPS = 4
NEG = float("-inf")


def kernel(sizes, cfg, q_hbm, k_hbm, v_hbm, lk_hbm, lv_hbm, sel_ref, out_ref,
           qbuf, kbuf, vbuf, send, recv, qsem, ksem, vsem, send_sem, recv_sem):
    positions, batch, local_blocks, heads, width, drafts, columns = cfg
    nx, ny, nz = sizes
    count = nx * ny * nz
    me = (lax.axis_index("gx") * ny + lax.axis_index("gy")) * nz + lax.axis_index("gz")
    per_head = width // LANES
    tiles = heads * per_head
    sharers = LANES // columns
    rows = batch * drafts
    tokens = positions * batch
    group_heads = heads // GROUPS
    group_tiles = group_heads * per_head
    my_group = (me // sharers) // group_tiles
    scale = 1.0 / math.sqrt(width)

    def device_of(d):
        return {"gx": d // (ny * nz), "gy": (d // nz) % ny, "gz": d % nz}

    def group_at(step):
        return lax.rem(my_group + 1 + step, GROUPS)

    for step in range(GROUPS):
        g = group_at(step)

        def start(i, _, g=g, step=step):
            c = g * group_tiles + i
            cols = pl.ds(pl.multiple_of(c * LANES, LANES), LANES)
            pltpu.make_async_copy(q_hbm.at[:, :, cols], qbuf.at[c], qsem.at[step]).start()
            pltpu.make_async_copy(lk_hbm.at[:, :, cols], kbuf.at[c, pl.ds(positions, local_blocks)], ksem.at[step]).start()
            pltpu.make_async_copy(k_hbm.at[:, :, cols], kbuf.at[c, pl.ds(0, positions)], ksem.at[step]).start()
            pltpu.make_async_copy(lv_hbm.at[:, :, cols], vbuf.at[c, pl.ds(positions, local_blocks)], vsem.at[step]).start()
            pltpu.make_async_copy(v_hbm.at[:, :, cols], vbuf.at[c, pl.ds(0, positions)], vsem.at[step]).start()
            return 0

        lax.fori_loop(0, group_tiles, start, 0)

    barrier = pltpu.get_barrier_semaphore()

    def greet(i, _):
        pl.semaphore_signal(barrier, inc=1, device_id=device_of(lax.rem(me + i, count)), device_id_type=pl.DeviceIdType.MESH)
        return 0

    lax.fori_loop(1, count, greet, 0)

    total_rows = tokens + local_blocks * batch
    block_cols = tokens // local_blocks
    same = (lax.broadcasted_iota(jnp.int32, (rows, block_cols), 1) % batch
            == lax.broadcasted_iota(jnp.int32, (rows, block_cols), 0) // drafts)
    same_lm = same[:, :local_blocks * batch]
    lm_bias = jnp.where(same_lm, 0.0, NEG)
    lane = lax.broadcasted_iota(jnp.int32, (rows, LANES), 1)
    row = lax.broadcasted_iota(jnp.int32, (rows, LANES), 0)

    def compute(step, _):
        g = group_at(step)
        span = pl.ds(g * group_tiles, group_tiles)
        pltpu.make_async_copy(qbuf.at[span], qbuf.at[span], qsem.at[step]).wait()
        pltpu.make_async_copy(kbuf.at[span], kbuf.at[span], ksem.at[step]).wait()
        probs = []
        stats = []
        for i in range(group_heads):
            h = g * group_heads + i
            q = jnp.concatenate([qbuf[h * per_head + c].reshape(rows, LANES) for c in range(per_head)], axis=1)
            k = jnp.concatenate([kbuf[h * per_head + c].reshape(total_rows, LANES) for c in range(per_head)], axis=1)
            s = lax.dot_general(q, k, (((1,), (1,)), ((), ())), preferred_element_type=jnp.float32) * scale
            chosen = jnp.concatenate(
                [jnp.broadcast_to(sel_ref[b, pl.ds(h, 1), :], (drafts, sel_ref.shape[2])) for b in range(batch)], axis=0)
            parts = []
            for j in range(local_blocks):
                hit = jnp.max(jnp.where(chosen == me * local_blocks + j, 1, 0), axis=1, keepdims=True)
                parts.append(jnp.where(same & (hit > 0), 0.0, NEG))
            s = s + jnp.concatenate(parts + [lm_bias], axis=1)
            peak = jnp.max(s, axis=1, keepdims=True)
            w = jnp.exp(s - peak)
            total = jnp.sum(w, axis=1, keepdims=True)
            probs.append(w.astype(jnp.bfloat16))
            spread = jnp.where(lane == row, peak, jnp.where(lane == row + rows, total, 0.0))
            stats.append(jnp.sum(spread, axis=0, keepdims=True))
        pltpu.make_async_copy(vbuf.at[span], vbuf.at[span], vsem.at[step]).wait()
        for i in range(group_heads):
            h = g * group_heads + i
            v = jnp.concatenate([vbuf[h * per_head + c].reshape(total_rows, LANES) for c in range(per_head)], axis=1)
            o = jnp.dot(probs[i], v, preferred_element_type=jnp.float32)
            for c in range(per_head):
                u = h * per_head + c
                send[u, pl.ds(0, rows), :] = o[:, c * LANES:(c + 1) * LANES]
                send[u, pl.ds(rows, 8), :] = jnp.broadcast_to(stats[i], (8, LANES))

        @pl.when(step == 0)
        def _():
            pl.semaphore_wait(barrier, count - 1)

        def post(i, _):
            d = g * group_tiles * sharers + i
            u = d // sharers

            @pl.when(d == me)
            def _():
                pltpu.make_async_copy(send.at[u], recv.at[me], recv_sem).start()

            @pl.when(d != me)
            def _():
                pltpu.make_async_remote_copy(
                    src_ref=send.at[u], dst_ref=recv.at[me], send_sem=send_sem, recv_sem=recv_sem,
                    device_id=device_of(d), device_id_type=pl.DeviceIdType.MESH).start()
            return 0

        lax.fori_loop(0, group_tiles * sharers, post, 0)
        return 0

    lax.fori_loop(0, GROUPS, compute, 0)

    pltpu.make_async_copy(recv, recv, recv_sem).wait()
    gathered = recv[:, rows, :]
    flipped = gathered.T
    peaks = flipped[:rows]
    totals = flipped[rows:2 * rows]
    top = jnp.max(peaks, axis=1, keepdims=True)
    factor = jnp.exp(peaks - top)
    denominator = jnp.sum(factor * totals, axis=1, keepdims=True)
    numerator = jnp.zeros((rows, LANES), jnp.float32)
    for s in range(count):
        numerator = numerator + factor[:, s:s + 1] * recv[s, pl.ds(0, rows), :]
    out_ref[...] = (numerator / denominator).reshape(batch, drafts, LANES)
    others = pl.ds(0, count - 1)
    pltpu.make_async_copy(recv.at[others], recv.at[others], send_sem).wait()


def body(sizes, query, keys, values, lm_keys, lm_values, selected):
    positions, batch, feature = keys.shape
    local_blocks = lm_keys.shape[0]
    heads = selected.shape[1]
    width = feature // heads
    drafts = query.shape[1]
    count = math.prod(sizes)
    columns = feature // count
    tiles = feature // LANES
    rows = batch * drafts
    cfg = (positions, batch, local_blocks, heads, width, drafts, columns)
    anywhere = pl.BlockSpec(memory_space=pl.ANY)
    vmem = pl.BlockSpec(memory_space=pltpu.VMEM)
    span = positions + local_blocks
    out = pl.pallas_call(
        functools.partial(kernel, sizes, cfg),
        out_shape=jax.ShapeDtypeStruct((batch, drafts, LANES), jnp.float32),
        in_specs=[anywhere] * 5 + [vmem],
        out_specs=vmem,
        scratch_shapes=[
            pltpu.VMEM((tiles, batch, drafts, LANES), jnp.bfloat16),
            pltpu.VMEM((tiles, span, batch, LANES), jnp.bfloat16),
            pltpu.VMEM((tiles, span, batch, LANES), jnp.bfloat16),
            pltpu.VMEM((tiles, rows + 8, LANES), jnp.float32),
            pltpu.VMEM((count, rows + 8, LANES), jnp.float32),
            pltpu.SemaphoreType.DMA((GROUPS,)),
            pltpu.SemaphoreType.DMA((GROUPS,)),
            pltpu.SemaphoreType.DMA((GROUPS,)),
            pltpu.SemaphoreType.DMA,
            pltpu.SemaphoreType.DMA,
        ],
        compiler_params=pltpu.CompilerParams(collective_id=0, has_side_effects=True),
        name="block_attention",
    )(query, keys, values, lm_keys, lm_values, selected)
    if columns < LANES:
        me = lax.axis_index(AXES)
        out = lax.dynamic_slice_in_dim(out, (me * columns) % LANES, columns, 2)
    return out


def solution(mesh):
    sizes = tuple(mesh.shape[a] for a in AXES)
    split = P(AXES, None, None)
    return jax.shard_map(
        functools.partial(body, sizes),
        mesh=mesh,
        in_specs=(P(), split, split, split, split, P()),
        out_specs=P(None, None, AXES),
        check_vma=False,
    )
```

```python
import functools
import math

import jax
import jax.numpy as jnp
from jax import lax
from jax.experimental import pallas as pl
from jax.experimental.pallas import tpu as pltpu
from jax.sharding import PartitionSpec as P

AXES = ("gx", "gy", "gz")
LANES = 128
NEG = float("-inf")


def kernel(sizes, pair, cfg, q_hbm, k_hbm, v_hbm, lk_hbm, lv_hbm, sel_ref, out_ref,
           qbuf, kbuf, vbuf, send, merged, recv, swap, qsem, ksem, vsem, pair_send, pair_recv, send_sem, recv_sem):
    positions, batch, local_blocks, heads, width, drafts, columns = cfg
    nx, ny, nz = sizes
    count = nx * ny * nz
    half = count // 2
    me = (lax.axis_index("gx") * ny + lax.axis_index("gy")) * nz + lax.axis_index("gz")
    stride = math.prod(sizes[pair + 1:])
    side = lax.rem(lax.axis_index(AXES[pair]), 2)
    my_slot = me // (2 * stride) * stride + lax.rem(me, stride)
    per_head = width // LANES
    tiles = heads * per_head
    sharers = LANES // columns
    side_tiles = stride // sharers
    group_tiles = 2 * side_tiles
    groups = tiles // group_tiles
    group_heads = group_tiles // per_head
    side_heads = side_tiles // per_head
    rows = batch * drafts
    tokens = positions * batch
    my_group = (me // sharers) // group_tiles
    scale = 1.0 / math.sqrt(width)
    mesh_ids = pl.DeviceIdType.MESH

    def device_of(d):
        return {"gx": d // (ny * nz), "gy": (d // nz) % ny, "gz": d % nz}

    def group_at(step):
        return lax.rem(my_group + 1 + step, groups)

    barrier = pltpu.get_barrier_semaphore()
    partner = {AXES[pair]: lax.axis_index(AXES[pair]) + 1 - 2 * side}
    pl.semaphore_signal(barrier, inc=1, device_id=partner, device_id_type=mesh_ids)

    def greet(i, _):
        slot = lax.rem(my_slot + i, half)
        d = slot // stride * (2 * stride) + side * stride + lax.rem(slot, stride)
        pl.semaphore_signal(barrier, inc=1, device_id=device_of(d), device_id_type=mesh_ids)
        return 0

    for step in range(groups):
        g = group_at(step)

        def start(i, _, g=g, step=step):
            c = g * group_tiles + i
            cols = pl.ds(pl.multiple_of(c * LANES, LANES), LANES)
            pltpu.make_async_copy(q_hbm.at[:, :, cols], qbuf.at[c], qsem.at[step]).start()
            pltpu.make_async_copy(lk_hbm.at[:, :, cols], kbuf.at[c, pl.ds(positions, local_blocks)], ksem.at[step]).start()
            pltpu.make_async_copy(k_hbm.at[:, :, cols], kbuf.at[c, pl.ds(0, positions)], ksem.at[step]).start()
            pltpu.make_async_copy(lv_hbm.at[:, :, cols], vbuf.at[c, pl.ds(positions, local_blocks)], vsem.at[step]).start()
            pltpu.make_async_copy(v_hbm.at[:, :, cols], vbuf.at[c, pl.ds(0, positions)], vsem.at[step]).start()
            return 0

        lax.fori_loop(0, group_tiles, start, 0)
        if step == 0:
            lax.fori_loop(1, half, greet, 0)

    total_rows = tokens + local_blocks * batch
    block_cols = tokens // local_blocks
    same = (lax.broadcasted_iota(jnp.int32, (rows, block_cols), 1) % batch
            == lax.broadcasted_iota(jnp.int32, (rows, block_cols), 0) // drafts)
    lm_bias = jnp.where(same[:, :local_blocks * batch], 0.0, NEG)
    lane = lax.broadcasted_iota(jnp.int32, (rows, LANES), 1)
    row = lax.broadcasted_iota(jnp.int32, (rows, LANES), 0)

    def stat_row(peak, total):
        spread = jnp.where(lane == row, peak, jnp.where(lane == row + rows, total, 0.0))
        return jnp.sum(spread, axis=0, keepdims=True)

    def stat_columns(line):
        line = jnp.broadcast_to(line, (rows, LANES))
        peak = jnp.sum(jnp.where(lane == row, line, 0.0), axis=1, keepdims=True)
        total = jnp.sum(jnp.where(lane == row + rows, line, 0.0), axis=1, keepdims=True)
        return peak, total

    def compute(step):
        g = group_at(step)
        span = pl.ds(g * group_tiles, group_tiles)
        pltpu.make_async_copy(qbuf.at[span], qbuf.at[span], qsem.at[step]).wait()
        pltpu.make_async_copy(kbuf.at[span], kbuf.at[span], ksem.at[step]).wait()
        probs = []
        stats = []
        for i in range(group_heads):
            h = g * group_heads + i
            q = jnp.concatenate([qbuf[h * per_head + c].reshape(rows, LANES) for c in range(per_head)], axis=1)
            k = jnp.concatenate([kbuf[h * per_head + c].reshape(total_rows, LANES) for c in range(per_head)], axis=1)
            s = lax.dot_general(q, k, (((1,), (1,)), ((), ())), preferred_element_type=jnp.float32) * scale
            chosen = jnp.concatenate(
                [jnp.broadcast_to(sel_ref[b, pl.ds(h, 1), :], (drafts, sel_ref.shape[2])) for b in range(batch)], axis=0)
            parts = []
            for j in range(local_blocks):
                hit = jnp.max(jnp.where(chosen == me * local_blocks + j, 1, 0), axis=1, keepdims=True)
                parts.append(jnp.where(same & (hit > 0), 0.0, NEG))
            s = s + jnp.concatenate(parts + [lm_bias], axis=1)
            peak = jnp.max(s, axis=1, keepdims=True)
            w = jnp.exp(s - peak)
            total = jnp.sum(w, axis=1, keepdims=True)
            probs.append(w.astype(jnp.bfloat16))
            stats.append(stat_row(peak, total))
        pltpu.make_async_copy(vbuf.at[span], vbuf.at[span], vsem.at[step]).wait()
        for i in range(group_heads):
            h = g * group_heads + i
            v = jnp.concatenate([vbuf[h * per_head + c].reshape(total_rows, LANES) for c in range(per_head)], axis=1)
            o = jnp.dot(probs[i], v, preferred_element_type=jnp.float32)
            for c in range(per_head):
                u = i * per_head + c
                send[step, u, pl.ds(0, rows), :] = o[:, c * LANES:(c + 1) * LANES]
                send[step, u, pl.ds(rows, 1), :] = stats[i]

    def swap_copy(step):
        return pltpu.make_async_remote_copy(
            src_ref=send.at[step, pl.ds((1 - side) * side_tiles, side_tiles)], dst_ref=swap.at[step],
            send_sem=pair_send.at[step], recv_sem=pair_recv.at[step],
            device_id=partner, device_id_type=mesh_ids)

    def merge(step):
        swap_copy(step).wait_recv()
        for i in range(side_heads):
            first = side * side_tiles + i * per_head
            peak0, total0 = stat_columns(send[step, first, pl.ds(rows, 1), :])
            peak1, total1 = stat_columns(swap[step, i * per_head, pl.ds(rows, 1), :])
            peak = jnp.maximum(peak0, peak1)
            factor0 = jnp.exp(peak0 - peak)
            factor1 = jnp.exp(peak1 - peak)
            line = stat_row(peak, factor0 * total0 + factor1 * total1)
            for c in range(per_head):
                u = i * per_head + c
                merged[step, u, pl.ds(0, rows), :] = (factor0 * send[step, first + c, pl.ds(0, rows), :]
                                                      + factor1 * swap[step, u, pl.ds(0, rows), :])
                merged[step, u, pl.ds(rows, 1), :] = line

    def post(step):
        base = (group_at(step) * group_tiles + side * side_tiles) * sharers

        def one(i, _):
            d = base + i
            u = i // sharers

            @pl.when(d == me)
            def _():
                recv[my_slot] = merged[step, u]

            @pl.when(d != me)
            def _():
                pltpu.make_async_remote_copy(
                    src_ref=merged.at[step, u], dst_ref=recv.at[my_slot], send_sem=send_sem, recv_sem=recv_sem,
                    device_id=device_of(d), device_id_type=mesh_ids).start()
            return 0

        lax.fori_loop(0, side_tiles * sharers, one, 0)

    for step in range(groups):
        compute(step)
        if step == 0:
            pl.semaphore_wait(barrier, half)
        swap_copy(step).start()
        if step > 0:
            merge(step - 1)
            post(step - 1)
    merge(groups - 1)
    post(groups - 1)

    others = pl.ds(0, half - 1)
    for step in range(groups):
        swap_copy(step).wait_send()
    pltpu.make_async_copy(recv.at[others], recv.at[others], send_sem).wait()
    pltpu.make_async_copy(recv.at[others], recv.at[others], recv_sem).wait()
    flipped = recv[:, rows, :].T
    peaks = flipped[:rows]
    totals = flipped[rows:2 * rows]
    top = jnp.max(peaks, axis=1, keepdims=True)
    factor = jnp.exp(peaks - top)
    denominator = jnp.sum(factor * totals, axis=1, keepdims=True)
    numerator = jnp.zeros((rows, LANES), jnp.float32)
    for s in range(half):
        numerator = numerator + factor[:, s:s + 1] * recv[s, pl.ds(0, rows), :]
    out_ref[...] = (numerator / denominator).reshape(batch, drafts, LANES)


def body(sizes, query, keys, values, lm_keys, lm_values, selected):
    positions, batch, feature = keys.shape
    local_blocks = lm_keys.shape[0]
    heads = selected.shape[1]
    width = feature // heads
    drafts = query.shape[1]
    count = math.prod(sizes)
    columns = min(feature // count, LANES)
    tiles = feature // LANES
    rows = batch * drafts
    cfg = (positions, batch, local_blocks, heads, width, drafts, columns)
    pair = sizes.index(max(sizes))
    stride = math.prod(sizes[pair + 1:])
    side_tiles = stride * columns // LANES
    groups = tiles // (2 * side_tiles)
    message = rows + 1
    anywhere = pl.BlockSpec(memory_space=pl.ANY)
    vmem = pl.BlockSpec(memory_space=pltpu.VMEM)
    span = positions + local_blocks
    out = pl.pallas_call(
        functools.partial(kernel, sizes, pair, cfg),
        out_shape=jax.ShapeDtypeStruct((batch, drafts, LANES), jnp.float32),
        in_specs=[anywhere] * 5 + [vmem],
        out_specs=vmem,
        scratch_shapes=[
            pltpu.VMEM((tiles, batch, drafts, LANES), jnp.bfloat16),
            pltpu.VMEM((tiles, span, batch, LANES), jnp.bfloat16),
            pltpu.VMEM((tiles, span, batch, LANES), jnp.bfloat16),
            pltpu.VMEM((groups, 2 * side_tiles, message, LANES), jnp.float32),
            pltpu.VMEM((groups, side_tiles, message, LANES), jnp.float32),
            pltpu.VMEM((count // 2, message, LANES), jnp.float32),
            pltpu.VMEM((groups, side_tiles, message, LANES), jnp.float32),
            pltpu.SemaphoreType.DMA((groups,)),
            pltpu.SemaphoreType.DMA((groups,)),
            pltpu.SemaphoreType.DMA((groups,)),
            pltpu.SemaphoreType.DMA((groups,)),
            pltpu.SemaphoreType.DMA((groups,)),
            pltpu.SemaphoreType.DMA,
            pltpu.SemaphoreType.DMA,
        ],
        compiler_params=pltpu.CompilerParams(collective_id=0, has_side_effects=True),
        name="block_attention",
    )(query, keys, values, lm_keys, lm_values, selected)
    if columns < LANES:
        me = lax.axis_index(AXES)
        out = lax.dynamic_slice_in_dim(out, (me * columns) % LANES, columns, 2)
    return out


def solution(mesh):
    sizes = tuple(mesh.shape[a] for a in AXES)
    split = P(AXES, None, None)
    return jax.shard_map(
        functools.partial(body, sizes),
        mesh=mesh,
        in_specs=(P(), split, split, split, split, P()),
        out_specs=P(None, None, AXES),
        check_vma=False,
    )
```
